32 devices in a mesh: parts: 2 (over y), blk: 4 (over x, core), sub: 4 (over z).
Axes of the slice: x: 2, y: 2, z: 4, core: 2. Of those that a mesh axis runs over, the one named last changes fastest.
Arguments:
- tokens: bfloat16 [256, 4096], P(('parts', 'blk'), 'sub'), parts along dimension 0, may hold values from -6 to 6
- expert_ids: int32 [256, 2], P(('parts', 'blk')), parts along dimension 0, may hold values from 0 to 7, all different within a row; in each aligned block of 32 rows (0 to 31, 32 to 63, ...) at most 16 rows name the same one
- gate_level: int32 [256, 2], P(('parts', 'blk')), parts along dimension 0, may hold values from 0 to 15
- gate_weight: bfloat16 [8, 4096, 8192], P('blk', None, 'sub'), may hold values from -0.09375 to 0.09375
- up_weight: bfloat16 [8, 4096, 8192], P('blk', None, 'sub'), may hold values from -0.09375 to 0.09375
- down_weight: bfloat16 [8, 8192, 4096], P('blk', 'sub'), may hold values from -0.0625 to 0.0625
Outputs:
- mixed_out: bfloat16 [256, 4096], P(('parts', 'blk'), 'sub'), parts along dimension 0
The draws below stay inside these ranges and needn't reach their ends.
There are 2 independent parts, one for each index of `parts`. The reference program is written for one: setup_inputs(seed, part) draws one part's arguments, and reference() takes and returns one part's arrays. A program takes and returns all parts, laid end to end along the dimension named above; an argument that names none is the same for every part. Nothing has to cross between parts.
Inputs may be any that keep to these rules, and one draw needn't show every extreme that they name: `expert_ids`: A token's 2 experts differ. Among the 32 tokens of one index of blk (aligned blocks of tokens), no expert is picked by more than 16 tokens, and in some block some expert is picked by exactly 16.
All inputs are finite; a program needn't handle non-finite values.
Results may differ from the reference program's by a relative error of at most 0.015.
Values may be sent and summed in bfloat16 or wider, within the bound.
No kernel may reach another device: no remote copies, remote signals or barrier semaphores. Data moves between devices by JAX's collectives and lax.ppermute only.
A program may use at most 192 MiB of HBM per device.

```python
import math
import jax
import jax.numpy as jnp
import numpy as np
from jax import lax

D = 4096
E = 8
TOP = 2
FF = 8192
LEVELS = 16
TOK_BLK = 32
FSPLIT = 1
SLOTS = 8
SLOT_FF = 8192
CAP = 16
TOKENS = 128
N_BLK = 4


def with_ends(array, rng, smallest, high):
    longest = array.shape.index(max(array.shape))
    spots = []
    for shift in (0, 1):
        where = [jax.random.randint(jax.random.fold_in(rng, axis), (), 0, length) for axis, length in enumerate(array.shape)]
        where[longest] = (where[longest] + shift) % array.shape[longest]
        spots.append(tuple(where))
    return array.at[spots[0]].set(smallest).at[spots[1]].set(high)


def steps_of(stream_key, shape, split, smallest, high):
    def one(dim, parts):
        draws = jax.random.uniform(jax.random.fold_in(jax.random.fold_in(stream_key, 6), dim), (parts,), jnp.float32, smallest / len(split), high / len(split))
        return jnp.repeat(jnp.exp(draws), shape[dim] // parts).reshape((-1,) + (1,) * (len(shape) - dim - 1))

    level = one(*split[0])
    for cut in split[1:]:
        level = level * one(*cut)
    return level


def routed_block(key, own, number, rows, amount, top, bound, slope):
    order = jax.random.permutation(key, amount)
    crowded, ordinary = load_shares(amount, rows * top, bound, slope, True), load_shares(amount, rows * top, bound, slope, False)
    places = jnp.arange(amount)

    def named(sizes, rotation):
        used = int((sizes > 0).sum())
        fixed = max(1, used // 4)
        passed = fixed + (places - fixed + rotation * (used - fixed)) % max(1, amount - fixed)
        return jnp.zeros((amount,), jnp.int32).at[order[jnp.where(places < fixed, places, passed)]].set(jnp.asarray(sizes, jnp.int32))

    sizes = jnp.where(number % 4 == 0, named(crowded, number // 4), named(ordinary, number - number // 4 - 1))
    mixed = jax.random.permutation(jax.random.fold_in(own, 3), amount)
    source_of, sink = mixed[0:amount // 2 * 2:2], mixed[1:amount // 2 * 2:2]
    room = jnp.minimum(sizes[source_of] - 1, bound - sizes[sink]) // 2
    room = jnp.where((source_of == order[0]) | (sink == order[0]) | (sizes[sink] == 0), 0, jnp.maximum(room, 0))
    passed = jax.random.randint(jax.random.fold_in(own, 4), (amount // 2,), 0, 1 << 20) % (room + 1)
    sizes = sizes.at[source_of].add(-passed).at[sink].add(passed)
    labels = jnp.searchsorted(jnp.cumsum(sizes), jnp.arange(rows * top), side="right").astype(jnp.int32)
    listing = labels.reshape(top, rows).T
    listing = listing[jax.random.permutation(jax.random.fold_in(own, 1), rows)]
    rotation = jax.random.randint(jax.random.fold_in(own, 2), (rows, 1), 0, top)
    return jnp.take_along_axis(listing, (jnp.arange(top)[None, :] + rotation) % top, axis=1)


def load_shares(count, total, bound, slope, full):
    weights = [(1 << 20) // math.isqrt(rank ** slope) + 1 for rank in range(1, count + 1)]
    largest = bound if full else min(bound, max(-(-total // count), total * weights[0] // sum(weights)))
    least = 1 if total - largest >= count - 1 else 0
    holding, surplus = [largest] + [least] * (count - 1), total - largest - least * (count - 1)
    while surplus > 0:
        free = [i for i in range(1, count) if holding[i] < largest] or [i for i in range(1, count) if holding[i] < bound]
        pool, budget = sum([weights[i] for i in free]), surplus
        for i in free:
            extra = min(bound - holding[i], max(1, budget * weights[i] // pool), surplus)
            holding[i] = holding[i] + extra
            surplus = surplus - extra
    return np.array(holding)


def centred(key, extent, spread, most, shards=(), kind=jnp.bfloat16):
    entries = jax.random.normal(key, extent, jnp.float32) * spread
    if len(shards) > 0:
        entries = steps_of(key, extent, shards, -0.22, 0.18) * entries
    return jnp.clip(entries, min=-most, max=most).astype(kind)


def setup_inputs(seed: int = 0, part: int = 0) -> dict:
    streams_of = jax.random.split(jax.random.key(seed), 7)
    part_splits = jax.random.split(jax.random.fold_in(streams_of[6], part), 7)
    tokens = centred(part_splits[0], (TOKENS, D), 1.0, 6.0, ((0, 4), (1, 4)))
    expert_ids_keys = jax.random.split(jax.random.fold_in(part_splits[1], 1), TOKENS // TOK_BLK)
    expert_ids_turns = jax.random.permutation(jax.random.fold_in(part_splits[1], 3), TOKENS // TOK_BLK)
    expert_ids = jax.vmap(lambda own, number: routed_block(jax.random.fold_in(part_splits[1], 2), own, number, TOK_BLK, E, TOP, CAP, 2))(expert_ids_keys, expert_ids_turns).reshape((TOKENS, TOP))
    gate_level = with_ends(jax.random.randint(part_splits[2], (TOKENS, TOP), 0, LEVELS), jax.random.fold_in(part_splits[2], 1), 0, LEVELS - 1).astype(jnp.int32)
    gate_weight = centred(streams_of[3], (SLOTS, D, SLOT_FF), D ** -0.5, 0.09375, ((0, 4), (2, 4)))
    up_weight = centred(streams_of[4], (SLOTS, D, SLOT_FF), D ** -0.5, 0.09375, ((0, 4), (2, 4)))
    down_weight = centred(streams_of[5], (SLOTS, SLOT_FF, D), FF ** -0.5, 0.0625, ((0, 4), (1, 4)))
    return {"tokens": tokens, "expert_ids": expert_ids, "gate_level": gate_level, "gate_weight": gate_weight, "up_weight": up_weight, "down_weight": down_weight}


def reference(tokens, expert_ids, gate_level, gate_weight, up_weight, down_weight):
    picked = expert_ids.reshape(N_BLK, TOK_BLK * TOP)
    onehot = (picked[:, :, None] == jnp.arange(E, dtype=jnp.int32)[None, None, :]).astype(jnp.int32)
    ranking = jnp.sum((jnp.cumsum(onehot, axis=1) - onehot) * onehot, axis=2)
    block_index = jnp.arange(N_BLK, dtype=jnp.int32)[:, None]
    position = (block_index * CAP + ranking).reshape(-1).astype(jnp.int32)
    flat_expert = expert_ids.reshape(-1).astype(jnp.int32)
    token_index = jnp.repeat(jnp.arange(TOKENS, dtype=jnp.int32), TOP)
    row_table = jnp.full((E, N_BLK * CAP), TOKENS, jnp.int32).at[flat_expert, position].set(token_index)
    padded = jnp.concatenate([tokens, jnp.zeros((1, D), tokens.dtype)], axis=0)

    def one_slot(slot_index):
        expert = slot_index % E
        slot_rows = padded[row_table[expert]]
        gate_acts = jnp.dot(slot_rows, gate_weight[slot_index], preferred_element_type=jnp.float32)
        up_acts = jnp.dot(slot_rows, up_weight[slot_index], preferred_element_type=jnp.float32)
        hidden = (jax.nn.silu(gate_acts) * up_acts).astype(jnp.bfloat16)
        return jnp.dot(hidden, down_weight[slot_index], preferred_element_type=jnp.float32).astype(jnp.bfloat16)

    slot_out = lax.map(one_slot, jnp.arange(SLOTS, dtype=jnp.int32))
    expert_sum = jnp.sum(slot_out.astype(jnp.float32).reshape(FSPLIT, E, N_BLK * CAP, D), axis=0)
    levels = gate_level.astype(jnp.float32) + 1.0
    shares = levels / jnp.sum(levels, axis=1, keepdims=True)
    gathered = expert_sum[flat_expert, position].reshape(TOKENS, TOP, D)
    mixed_out = jnp.sum(gathered * shares[:, :, None], axis=1)
    return mixed_out.astype(jnp.bfloat16)
```

```python
import functools

import jax
import jax.numpy as jnp
from jax import lax
from jax.experimental import pallas as pl
from jax.experimental.pallas import tpu as pltpu
from jax.sharding import PartitionSpec as P

E = 8
HELD = 4
LANES = 128
MIB = 1 << 20
VMEM = pl.BlockSpec(memory_space=pltpu.VMEM)
HBM = pl.BlockSpec(memory_space=pltpu.HBM)
SMEM = pl.BlockSpec(memory_space=pltpu.SMEM)


def params(mib):
    return pltpu.CompilerParams(vmem_limit_bytes=mib * MIB)


def cost(flops, moved):
    return pl.CostEstimate(flops=int(flops), bytes_accessed=int(moved), transcendentals=0)


def swap(value, axis, distance):
    count = lax.axis_size(axis)
    return lax.ppermute(value, axis, [(i, i ^ distance) for i in range(count)])


def bits_of(count):
    width = count.bit_length() - 1
    assert 1 << width == count
    return [1 << i for i in range(width)]


def spread(value):
    held = {0: value}
    for bit in reversed(bits_of(lax.axis_size("blk"))):
        for near in list(held):
            held[near ^ bit] = swap(held[near], "blk", bit)
    return list(held.values())


def share_kernel(ids_ref, level_ref, share_ref):
    levels = level_ref[...].astype(jnp.float32) + 1.0
    shares = levels / jnp.sum(levels, axis=1, keepdims=True)
    ids = ids_ref[...]
    lane = lax.broadcasted_iota(jnp.int32, (ids.shape[0], LANES), 1)
    table = jnp.zeros((ids.shape[0], LANES), jnp.float32)
    for k in range(ids.shape[1]):
        table = table + jnp.where(lane == ids[:, k : k + 1], shares[:, k : k + 1], 0.0)
    share_ref[...] = table


def fetch_kernel(weight_ref, after_ref, held_ref, sems, *, slot, column):
    pieces = sems.shape[0]
    depth = held_ref.shape[0] // pieces
    copies = []
    for i in range(pieces):
        rows = pl.ds(i * depth, depth)
        source = weight_ref.at[slot, rows, pl.ds(column, held_ref.shape[1])]
        copies.append(pltpu.make_async_copy(source, held_ref.at[rows], sems.at[i]))
    for copy in copies:
        copy.start()
    for copy in copies:
        copy.wait()


def fetch(weight, slot, column, width, after):
    depth = weight.shape[1]
    return pl.pallas_call(
        functools.partial(fetch_kernel, slot=slot, column=column),
        out_shape=pltpu.VMEM((depth, width), jnp.bfloat16),
        in_specs=[HBM, pl.BlockSpec(memory_space=pl.ANY)],
        out_specs=VMEM,
        scratch_shapes=[pltpu.SemaphoreType.DMA((8,))],
        compiler_params=params(1),
        cost_estimate=cost(1e9, 4 * depth * width),
    )(weight, after)


def hidden_kernel(sub_ref, *refs, blocks, chunks, held):
    count = blocks * chunks
    pieces, refs = refs[:count], refs[count:]
    gate_ref, up_ref, refs = refs[0], refs[1], refs[2:]
    kept, refs = dict(zip(held, refs[: len(held)])), refs[len(held) :]
    hidden_ref, gathered, ring, sems = refs
    slots, _, width = gate_ref.shape
    rows, features = pieces[0].shape
    depth, _, tile = ring.shape
    wanted = [
        (which, slot, column)
        for column in range(0, width, tile)
        for slot in range(slots)
        for which in range(2)
        if not any(
            key[:2] == (which, slot) and key[2] <= column < key[2] + ref.shape[1]
            for key, ref in kept.items()
        )
    ]

    def copy(index):
        which, slot, column = wanted[index]
        source = (gate_ref, up_ref)[which].at[slot, :, pl.ds(column, tile)]
        return pltpu.make_async_copy(source, ring.at[index % depth], sems.at[index % depth])

    for i in range(min(depth, len(wanted))):
        copy(i).start()
    for k in range(chunks):
        offset = pl.multiple_of((sub_ref[0] ^ k) * features, features)
        for j in range(blocks):
            gathered[j * rows : (j + 1) * rows, pl.ds(offset, features)] = pieces[k * blocks + j][...]
    for column in range(0, width, tile):
        for slot in range(slots):
            acts = []
            for which in range(2):
                if (which, slot, column) in wanted:
                    index = wanted.index((which, slot, column))
                    copy(index).wait()
                    block = ring[index % depth]
                else:
                    index = None
                    for key, ref in kept.items():
                        if key[:2] == (which, slot) and key[2] <= column < key[2] + ref.shape[1]:
                            block = ref[:, column - key[2] : column - key[2] + tile]
                acts.append(jnp.dot(gathered[...], block, preferred_element_type=jnp.float32))
                if index is not None and index + depth < len(wanted):
                    copy(index + depth).start()
            gate, up = acts
            hidden = gate / (1.0 + jnp.exp(-gate)) * up
            hidden_ref[slot, :, column : column + tile] = hidden.astype(jnp.bfloat16)


def down_kernel(where_ref, *refs, blocks):
    shares = refs[:blocks]
    hidden_ref, weight_ref, keep_ref, send_ref = refs[blocks:]
    slots = hidden_ref.shape[0]
    rows = shares[0].shape[0]
    half = keep_ref.shape[0]
    table = jnp.concatenate([s[...] for s in shares], axis=0)
    lane = lax.broadcasted_iota(jnp.int32, table.shape, 1)
    total = None
    for n in range(slots):
        expert = lax.rem(where_ref[1] * slots + n, E)
        share = jnp.sum(jnp.where(lane == expert, table, 0.0), axis=1, keepdims=True)
        part = jnp.dot(hidden_ref[n], weight_ref[n], preferred_element_type=jnp.float32)
        part = jnp.where(share > 0.0, share * part, 0.0)
        total = part if total is None else total + part
    keep_ref[...] = total[:half]
    send_ref[...] = total[half:].astype(jnp.bfloat16)


def half_kernel(keep_ref, got_ref, low_ref, high_ref):
    half = low_ref.shape[0]
    total = keep_ref[...] + got_ref[...].astype(jnp.float32)
    low_ref[...] = total[:half]
    high_ref[...] = total[half:].astype(jnp.bfloat16)


def split_kernel(keep_ref, got_ref, *outs):
    total = keep_ref[...] + got_ref[...].astype(jnp.float32)
    width = outs[0].shape[1]
    for i, out in enumerate(outs):
        out[...] = total[:, i * width : (i + 1) * width].astype(out.dtype)


def last_kernel(own_ref, *refs):
    total = own_ref[...]
    for ref in refs[:-1]:
        total = total + ref[...].astype(jnp.float32)
    refs[-1][...] = total.astype(jnp.bfloat16)


def shards(tokens, expert_ids, gate_level, gate_weight, up_weight, down_weight):
    blocks = lax.axis_size("blk")
    chunks = lax.axis_size("sub")
    sub = lax.axis_index("sub").astype(jnp.int32)
    blk = lax.axis_index("blk").astype(jnp.int32)
    where = jnp.stack([sub, blk])
    slots, model, width = gate_weight.shape
    rows, features = tokens.shape
    total_rows = rows * blocks
    gate_weight, up_weight, down_weight = (
        pltpu.with_memory_space_constraint(w, pltpu.HBM) for w in (gate_weight, up_weight, down_weight)
    )
    weight_bytes = 2 * slots * model * width

    parts = [tokens] + [swap(tokens, "sub", k) for k in range(1, chunks)]
    pieces = []
    for part in parts:
        pieces += spread(part)

    table = pl.pallas_call(
        share_kernel,
        out_shape=jax.ShapeDtypeStruct((rows, LANES), jnp.float32),
        in_specs=[VMEM, VMEM],
        out_specs=VMEM,
        compiler_params=params(1),
    )(expert_ids, gate_level)
    shares = spread(table)

    tile = min(512, width)
    keep_width = max(tile, width // 2)
    plan = [
        (which, slot, column)
        for slot in range(slots)
        for column in range(0, width, keep_width)
        for which in range(2)
    ]
    plan = plan[:HELD]
    held = []
    for i, (which, slot, column) in enumerate(plan):
        weight = (gate_weight, up_weight)[which]
        after = parts[max(0, min(i - 1, len(parts) - 1))]
        held.append(fetch(weight, slot, column, keep_width, after))
    steps = 2 * slots * (width // tile) - len(plan) * (keep_width // tile)
    ring = max(1, min(2, steps))
    hidden = pl.pallas_call(
        functools.partial(hidden_kernel, blocks=blocks, chunks=chunks, held=plan),
        out_shape=pltpu.VMEM((slots, total_rows, width), jnp.bfloat16),
        in_specs=[SMEM] + [VMEM] * (blocks * chunks) + [HBM] * 2 + [VMEM] * len(plan),
        out_specs=VMEM,
        scratch_shapes=[
            pltpu.VMEM((total_rows, model), jnp.bfloat16),
            pltpu.VMEM((ring, model, tile), jnp.bfloat16),
            pltpu.SemaphoreType.DMA((ring,)),
        ],
        compiler_params=params(19),
        cost_estimate=cost(4 * total_rows * slots * model * width, weight_bytes),
    )(where, *pieces, gate_weight, up_weight, *held)

    group = max(1, chunks // 2)
    column_tile = min(256, features)
    per = features // column_tile
    stages = bits_of(blocks)
    half = total_rows // 2

    def down(offset):
        def weight_map(j, where):
            return (0, 0, (where[0] ^ (offset + j // per)) * per + lax.rem(j, per))

        columns = group * features
        keep, send = pl.pallas_call(
            functools.partial(down_kernel, blocks=blocks),
            grid_spec=pltpu.PrefetchScalarGridSpec(
                num_scalar_prefetch=1,
                grid=(group * per,),
                in_specs=[pl.BlockSpec((rows, LANES), lambda j, w: (0, 0))] * blocks
                + [
                    pl.BlockSpec((slots, total_rows, width), lambda j, w: (0, 0, 0)),
                    pl.BlockSpec((slots, width, column_tile), weight_map),
                ],
                out_specs=[
                    pl.BlockSpec((half, column_tile), lambda j, w: (0, j)),
                    pl.BlockSpec((half, column_tile), lambda j, w: (0, j)),
                ],
            ),
            out_shape=(
                jax.ShapeDtypeStruct((half, columns), jnp.float32),
                jax.ShapeDtypeStruct((half, columns), jnp.bfloat16),
            ),
            compiler_params=params(24),
            cost_estimate=cost(
                2 * total_rows * slots * columns * width, 2 * slots * columns * width
            ),
        )(where, *shares, hidden, down_weight)
        for stage, bit in enumerate(stages):
            got = swap(send, "blk", bit)
            size = keep.shape[0] // 2
            if stage + 1 < len(stages):
                keep, send = pl.pallas_call(
                    half_kernel,
                    out_shape=(
                        pltpu.VMEM((size, columns), jnp.float32),
                        pltpu.VMEM((size, columns), jnp.bfloat16),
                    ),
                    in_specs=[VMEM] * 2,
                    out_specs=(VMEM, VMEM),
                    compiler_params=params(4),
                    cost_estimate=cost(1e6, 6 * size * columns),
                )(keep, got)
            else:
                outs = [
                    pltpu.VMEM((rows, features), jnp.float32 if offset + i == 0 else jnp.bfloat16)
                    for i in range(group)
                ]
                return pl.pallas_call(
                    split_kernel,
                    out_shape=tuple(outs),
                    in_specs=[VMEM] * 2,
                    out_specs=(VMEM,) * group,
                    compiler_params=params(4),
                    cost_estimate=cost(1e6, 6 * rows * columns),
                )(keep, got)

    finals = {}
    for offset in reversed(range(0, chunks, group)):
        for i, piece in enumerate(down(offset)):
            k = offset + i
            finals[k] = swap(piece, "sub", k) if k else piece
    return pl.pallas_call(
        last_kernel,
        out_shape=jax.ShapeDtypeStruct((rows, features), jnp.bfloat16),
        in_specs=[VMEM] * chunks,
        out_specs=VMEM,
        compiler_params=params(4),
    )(*[finals[k] for k in range(chunks)])


def solution(mesh):
    return jax.shard_map(
        shards,
        mesh=mesh,
        in_specs=(
            P(("parts", "blk"), "sub"),
            P(("parts", "blk"), None),
            P(("parts", "blk"), None),
            P("blk", None, "sub"),
            P("blk", None, "sub"),
            P("blk", "sub", None),
        ),
        out_specs=P(("parts", "blk"), "sub"),
        check_vma=False,
    )
```
